32 devices in a mesh: batch: 4 (over y, x), cols: 8 (over z, core).
Axes of the slice: x: 2, y: 2, z: 4, core: 2. Of those that a mesh axis runs over, the one named last changes fastest.
Arguments:
- grad_query: float32 [4, 2048, 2048], P('batch', None, 'cols'), may hold values from -0.875 to 0.875
- grad_key: float32 [4, 2048, 2048], P('batch', None, 'cols'), may hold values from -0.875 to 0.875
- grad_value: float32 [4, 2048, 2048], P('batch', None, 'cols'), may hold values from -0.875 to 0.875
- grad_mixed: float32 [4, 2048, 2048], P('batch', 'cols'), may hold values from -0.875 to 0.875
- grad_norm: float32 [4, 2048], P('batch'), may hold values from -8 to 8
- grad_bias: float32 [4, 2048], P('batch'), may hold values from -8 to 8
- weight_query: float32 [2048, 2048], P('batch', 'cols'), may hold values from -0.1875 to 0.1875
- weight_key: float32 [2048, 2048], P('batch', 'cols'), may hold values from -0.1875 to 0.1875
- weight_value: float32 [2048, 2048], P('batch', 'cols'), may hold values from -0.1875 to 0.1875
- weight_mixed: float32 [2048, 2048], P('cols', 'batch'), may hold values from -0.1875 to 0.1875
- weight_norm: float32 [2048], P('batch'), may hold values from 0.25 to 1.75
- weight_bias: float32 [2048], P('batch'), may hold values from -3 to 3
Outputs:
- copy_query: bfloat16 [2048, 2048], P(None, 'cols')
- copy_key: bfloat16 [2048, 2048], P(None, 'cols')
- copy_value: bfloat16 [2048, 2048], P(None, 'cols')
- copy_mixed: bfloat16 [2048, 2048], P('cols')
- copy_norm: bfloat16 [2048], replicated
- copy_bias: bfloat16 [2048], replicated
- new_query: float32 [2048, 2048], P('batch', 'cols')
- new_key: float32 [2048, 2048], P('batch', 'cols')
- new_value: float32 [2048, 2048], P('batch', 'cols')
- new_mixed: float32 [2048, 2048], P('cols', 'batch')
- new_norm: float32 [2048], P('batch')
- new_bias: float32 [2048], P('batch')
The draws below stay inside these ranges and needn't reach their ends.
All inputs are finite; a program needn't handle non-finite values.
Results may differ from the reference program's by a relative error of at most 0.0004.
Values may be sent and summed in bfloat16 or wider, within the bound.
A program may use at most 64 MiB of HBM per device.

```python
import jax
import jax.numpy as jnp
from jax import lax

WIDTH = 2048
ATTN = 2048
REPLICAS = 4


def strengthened(entries, own_key, source, target, shards_of, factor):
    owner, partner = [(jnp.arange(entries.shape[position]) // (entries.shape[position] // shards_of)).reshape([-1 if axis == position else 1 for axis in range(entries.ndim)]) for position in (source, target)]
    chosen = jax.random.permutation(own_key, shards_of)[partner]
    strong = (owner == chosen) | (owner == (partner + shards_of // 2) % shards_of)
    return jnp.where(strong, factor * entries, entries)


def block_scale(key, shape, split, low, largest):
    level, own = 1.0, jax.random.fold_in(key, 6)
    for position, parts in split:
        steps = jnp.exp(jax.random.uniform(jax.random.fold_in(own, position), (parts,), jnp.float32, low / len(split), largest / len(split)))
        level = level * jnp.repeat(steps, shape[position] // parts).reshape([-1 if axis == position else 1 for axis in range(len(shape))])
    return level


def bell_draw(rng, extent, deviation, bound, cuts=(), held_as=jnp.bfloat16):
    values = jax.random.normal(rng, extent, jnp.float32) * deviation
    if len(cuts) > 0:
        values = block_scale(rng, extent, cuts, -0.22, 0.18) * values
    return jnp.clip(values, min=-bound, max=bound).astype(held_as)


def bell_draw_with(key, shape, deviation, most, split, heavy, held_as=jnp.bfloat16):
    entries = deviation * jax.random.normal(key, shape, jnp.float32)
    if split:
        entries = entries * block_scale(key, shape, split, -0.22, 0.18)
    return jnp.clip(strengthened(entries, jax.random.fold_in(key, 3), *heavy), -most, most).astype(held_as)


def setup_inputs(seed: int = 0) -> dict:
    seeds = jax.random.split(jax.random.key(seed), 13)
    grad_query = bell_draw_with(seeds[0], (REPLICAS, WIDTH, ATTN), 0.1, 0.875, ((0, 4), (2, 8)), (0, 1, 4, 2.0), jnp.float32)
    grad_key = bell_draw_with(seeds[1], (REPLICAS, WIDTH, ATTN), 0.1, 0.875, ((0, 4), (2, 8)), (0, 1, 4, 2.0), jnp.float32)
    grad_value = bell_draw_with(seeds[2], (REPLICAS, WIDTH, ATTN), 0.1, 0.875, ((0, 4), (2, 8)), (0, 1, 4, 2.0), jnp.float32)
    grad_mixed = bell_draw_with(seeds[3], (REPLICAS, ATTN, WIDTH), 0.1, 0.875, ((0, 4), (1, 8)), (0, 2, 4, 2.0), jnp.float32)
    grad_norm = bell_draw_with(seeds[4], (REPLICAS, WIDTH), 1.0, 8.0, ((0, 4),), (0, 1, 4, 2.0), jnp.float32)
    grad_bias = bell_draw_with(seeds[5], (REPLICAS, WIDTH), 1.0, 8.0, ((0, 4),), (0, 1, 4, 2.0), jnp.float32)
    weight_query = bell_draw_with(seeds[6], (WIDTH, ATTN), WIDTH ** -0.5, 0.1875, ((0, 4), (1, 8)), (1, 0, 8, 2.0), jnp.float32)
    weight_key = bell_draw_with(seeds[7], (WIDTH, ATTN), WIDTH ** -0.5, 0.1875, ((0, 4), (1, 8)), (1, 0, 8, 2.0), jnp.float32)
    weight_value = bell_draw_with(seeds[8], (WIDTH, ATTN), WIDTH ** -0.5, 0.1875, ((0, 4), (1, 8)), (1, 0, 8, 2.0), jnp.float32)
    weight_mixed = bell_draw_with(seeds[9], (ATTN, WIDTH), ATTN ** -0.5, 0.1875, ((0, 8), (1, 4)), (0, 1, 8, 2.0), jnp.float32)
    weight_norm = jnp.clip(1.0 + 0.15 * jax.random.normal(seeds[10], (WIDTH,), jnp.float32), 0.25, 1.75)
    weight_bias = bell_draw(seeds[11], (WIDTH,), 0.5, 3.0, ((0, 4),), jnp.float32)
    return dict(grad_query=grad_query, grad_key=grad_key, grad_value=grad_value, grad_mixed=grad_mixed, grad_norm=grad_norm, grad_bias=grad_bias, weight_query=weight_query, weight_key=weight_key, weight_value=weight_value, weight_mixed=weight_mixed, weight_norm=weight_norm, weight_bias=weight_bias)


learn_rate = 0.4

def reference(grad_query, grad_key, grad_value, grad_mixed, grad_norm, grad_bias, weight_query, weight_key, weight_value, weight_mixed, weight_norm, weight_bias):
    mean_query = lax.optimization_barrier(jnp.sum(grad_query.astype(jnp.float32), axis=0)) * REPLICAS ** (-0.5)
    mean_key = lax.optimization_barrier(jnp.sum(grad_key.astype(jnp.float32), axis=0)) * REPLICAS ** (-0.5)
    mean_value = lax.optimization_barrier(jnp.sum(grad_value.astype(jnp.float32), axis=0)) * REPLICAS ** (-0.5)
    mean_mixed = lax.optimization_barrier(jnp.sum(grad_mixed.astype(jnp.float32), axis=0)) * REPLICAS ** (-0.5)
    mean_norm = lax.optimization_barrier(jnp.sum(grad_norm.astype(jnp.float32), axis=0)) * REPLICAS ** (-0.5)
    mean_bias = lax.optimization_barrier(jnp.sum(grad_bias.astype(jnp.float32), axis=0)) * REPLICAS ** (-0.5)
    ratio_query = jnp.sqrt(lax.optimization_barrier(jnp.sum(weight_query * weight_query, axis=1, keepdims=True))) * lax.rsqrt(lax.optimization_barrier(jnp.sum(mean_query * mean_query, axis=1, keepdims=True)) + 1e-06)
    mean_query = mean_query * ratio_query
    ratio_key = jnp.sqrt(lax.optimization_barrier(jnp.sum(weight_key * weight_key, axis=1, keepdims=True))) * lax.rsqrt(lax.optimization_barrier(jnp.sum(mean_key * mean_key, axis=1, keepdims=True)) + 1e-06)
    mean_key = mean_key * ratio_key
    ratio_value = jnp.sqrt(lax.optimization_barrier(jnp.sum(weight_value * weight_value, axis=1, keepdims=True))) * lax.rsqrt(lax.optimization_barrier(jnp.sum(mean_value * mean_value, axis=1, keepdims=True)) + 1e-06)
    mean_value = mean_value * ratio_value
    ratio_mixed = jnp.sqrt(lax.optimization_barrier(jnp.sum(weight_mixed * weight_mixed, axis=0, keepdims=True))) * lax.rsqrt(lax.optimization_barrier(jnp.sum(mean_mixed * mean_mixed, axis=0, keepdims=True)) + 1e-06)
    mean_mixed = mean_mixed * ratio_mixed
    new_query = weight_query - learn_rate * mean_query
    new_key = weight_key - learn_rate * mean_key
    new_value = weight_value - learn_rate * mean_value
    new_mixed = weight_mixed - learn_rate * mean_mixed
    new_norm = weight_norm - learn_rate * mean_norm
    new_bias = weight_bias - learn_rate * mean_bias
    copy_query = new_query.astype(jnp.bfloat16)
    copy_key = new_key.astype(jnp.bfloat16)
    copy_value = new_value.astype(jnp.bfloat16)
    copy_mixed = new_mixed.astype(jnp.bfloat16)
    copy_norm = new_norm.astype(jnp.bfloat16)
    copy_bias = new_bias.astype(jnp.bfloat16)
    return (copy_query, copy_key, copy_value, copy_mixed, copy_norm, copy_bias, new_query, new_key, new_value, new_mixed, new_norm, new_bias)
```

```python
import functools
import math

import jax
import jax.numpy as jnp
from jax import lax
from jax.experimental import pallas as pl
from jax.experimental.pallas import tpu as pltpu
from jax.sharding import PartitionSpec as P

learn_rate = 0.4
LANES = 128


def kernel(n, m, n_x, n_y, *refs):
    grads, small_grads = refs[0:4], refs[4:6]
    weights, small_weights = refs[6:10], refs[10:12]
    copies, news = refs[12:16], refs[16:20]
    small_full, small_own = refs[20:22]
    scratch = refs[22:]
    first_in, second_in, held = scratch[0:4], scratch[4:8], scratch[8:12]
    total, own_weight = scratch[12:16], scratch[16:20]
    squares, squares_in, small_grad_in, small_weight_in = scratch[20:24]
    (
        load_sem, weight_sem,
        first_send, first_recv, second_send, second_recv,
        square_send, square_recv, square_own,
        back_send, back_recv, spread_send, spread_recv,
        small_send, small_recv, small_local,
    ) = scratch[24:]
    rate = n ** (-0.5)

    me = lax.axis_index("batch")
    col = lax.axis_index("cols")
    y, x = me // n_x, lax.rem(me, n_x)

    def spot(half, d_first, d_second):
        if half == 0:
            return lax.rem(y + d_second, n_y) * n_x + lax.rem(x + d_first, n_x)
        return lax.rem(y + d_first, n_y) * n_x + lax.rem(x + d_second, n_x)

    def extents(half):
        return (n_x, n_y) if half == 0 else (n_y, n_x)

    def piece(a, ref, chunk, half):
        rows, columns = total[a].shape
        depth = rows // 2
        if a < 3:
            start = pl.multiple_of(chunk * rows + half * depth, depth)
            return ref.at[pl.ds(start, depth), :]
        start = pl.multiple_of(chunk * columns, columns)
        return ref.at[pl.ds(half * depth, depth), pl.ds(start, columns)]

    loads, weight_loads = {}, []
    for a in range(4):
        for half in range(2):
            for d in range(extents(half)[1]):
                loads[a, half, d] = pltpu.make_async_copy(
                    piece(a, grads[a].at[0], spot(half, 0, d), half),
                    held[a].at[half, d],
                    load_sem.at[a, half, d],
                )
        weight_loads.append(pltpu.make_async_copy(weights[a], own_weight[a], weight_sem.at[a]))
    small_loads = []
    for i in range(2):
        small_loads.append(pltpu.make_async_copy(small_grads[i], small_grad_in.at[me, i], small_local.at[i]))
        small_loads.append(pltpu.make_async_copy(small_weights[i], small_weight_in.at[me, i], small_local.at[2 + i]))

    barrier = pltpu.get_barrier_semaphore()
    for d in range(1, n):
        pl.semaphore_signal(barrier, inc=1, device_id={"batch": lax.rem(me + d, n)})
    for d in range(1, m):
        pl.semaphore_signal(barrier, inc=1, device_id={"cols": lax.rem(col + d, m)})
    for copy in weight_loads:
        copy.start()
    for copy in loads.values():
        copy.start()
    for copy in small_loads:
        copy.start()
    pl.semaphore_wait(barrier, n - 1 + m - 1)

    first = {}
    for a in range(4):
        for d_second in range(max(n_x, n_y) - 1, -1, -1):
            for half in range(2):
                n_first, n_second = extents(half)
                if d_second >= n_second:
                    continue
                for d_first in range(1, n_first):
                    copy = pltpu.make_async_remote_copy(
                        src_ref=piece(a, grads[a].at[0], spot(half, d_first, d_second), half),
                        dst_ref=first_in[a].at[half, d_first - 1, d_second],
                        send_sem=first_send.at[a, half, d_first - 1, d_second],
                        recv_sem=first_recv.at[a, half, d_first - 1, d_second],
                        device_id={"batch": spot(half, d_first, 0)},
                    )
                    copy.start()
                    first[a, half, d_first, d_second] = copy
        if a == 0:
            small = []
            for d in range(1, n):
                for i in range(2):
                    for k, (source, target) in enumerate(
                        ((small_grads[i], small_grad_in), (small_weights[i], small_weight_in))
                    ):
                        copy = pltpu.make_async_remote_copy(
                            src_ref=source,
                            dst_ref=target.at[me, i],
                            send_sem=small_send.at[d - 1, i, k],
                            recv_sem=small_recv.at[d - 1, i, k],
                            device_id={"batch": lax.rem(me + d, n)},
                        )
                        copy.start()
                        small.append(copy)

    def row_squares(a, value):
        value = value * value
        if a == 3:
            return jnp.sum(value, axis=0, keepdims=True)
        folded = value[:, :LANES]
        for start in range(LANES, value.shape[1], LANES):
            folded = folded + value[:, start : start + LANES]
        return jnp.sum(folded.T, axis=0, keepdims=True)

    for a in range(4):
        weight_loads[a].wait()
        squares[a, 0:1] = row_squares(a, own_weight[a][...])

    second = {}

    def add_first(a):
        for d_second in range(max(n_x, n_y) - 1, -1, -1):
            for half in range(2):
                n_first, n_second = extents(half)
                if d_second >= n_second:
                    continue
                loads[a, half, d_second].wait()
                value = held[a][half, d_second]
                for d_first in range(1, n_first):
                    first[a, half, d_first, d_second].wait_recv()
                    value = value + first_in[a][half, d_first - 1, d_second]
                held[a][half, d_second] = value
                if d_second > 0:
                    copy = pltpu.make_async_remote_copy(
                        src_ref=held[a].at[half, d_second],
                        dst_ref=second_in[a].at[half, d_second - 1],
                        send_sem=second_send.at[a, half, d_second - 1],
                        recv_sem=second_recv.at[a, half, d_second - 1],
                        device_id={"batch": spot(half, 0, d_second)},
                    )
                    copy.start()
                    second[a, half, d_second] = copy

    exchange = {}

    def add_second(a):
        depth = total[a].shape[0] // 2
        for half in range(2):
            value = held[a][half, 0]
            for d_second in range(1, extents(half)[1]):
                second[a, half, d_second].wait_recv()
                value = value + second_in[a][half, d_second - 1]
            total[a][half * depth : (half + 1) * depth] = value * rate
        squares[a, 1:2] = row_squares(a, total[a][...])
        own = pltpu.make_async_copy(squares.at[a], squares_in.at[a, col], square_own.at[a])
        exchange[a] = [own]
        for d in range(1, m):
            copy = pltpu.make_async_remote_copy(
                src_ref=squares.at[a],
                dst_ref=squares_in.at[a, col],
                send_sem=square_send.at[a, d - 1],
                recv_sem=square_recv.at[a, d - 1],
                device_id={"cols": lax.rem(col + d, m)},
            )
            copy.start()
            exchange[a].append(copy)
        own.start()

    back, spread = {}, {}

    def send_spread(a, half, d_second):
        n_first, n_second = extents(half)
        slab = piece(a, copies[a], spot(half, 0, n_second - d_second), half)
        for d_first in range(1, n_first):
            copy = pltpu.make_async_remote_copy(
                src_ref=slab,
                dst_ref=slab,
                send_sem=spread_send.at[a, half, d_first - 1, d_second],
                recv_sem=spread_recv.at[a, half, d_first - 1, d_second],
                device_id={"batch": spot(half, d_first, 0)},
            )
            copy.start()
            spread[a, half, d_first, d_second] = copy

    def update(a):
        exchange[a][0].wait()
        for copy in exchange[a][1:]:
            copy.wait_recv()
        both = squares_in[a, 0]
        for d in range(1, m):
            both = both + squares_in[a, d]
        ratio = learn_rate * (jnp.sqrt(both[0:1]) * lax.rsqrt(both[1:2] + 1e-06))
        rows, columns = total[a].shape
        if a < 3:
            ratio = jnp.broadcast_to(ratio, (LANES, rows)).T
            for start in range(0, columns, LANES):
                block = slice(start, start + LANES)
                news[a][:, block] = own_weight[a][:, block] - total[a][:, block] * ratio
        else:
            news[a][...] = own_weight[a][...] - total[a][...] * ratio
        depth = rows // 2
        for half in range(2):
            piece(a, copies[a], me, half)[...] = news[a][half * depth : (half + 1) * depth].astype(jnp.bfloat16)
        for half in range(2):
            slab = piece(a, copies[a], me, half)
            for d_second in range(1, extents(half)[1]):
                copy = pltpu.make_async_remote_copy(
                    src_ref=slab,
                    dst_ref=slab,
                    send_sem=back_send.at[a, half, d_second - 1],
                    recv_sem=back_recv.at[a, half, d_second - 1],
                    device_id={"batch": spot(half, 0, d_second)},
                )
                copy.start()
                back[a, half, d_second] = copy
            send_spread(a, half, 0)

    def pass_on(a):
        for half in range(2):
            for d_second in range(1, extents(half)[1]):
                back[a, half, d_second].wait_recv()
                send_spread(a, half, d_second)

    add_first(0)
    for copy in small_loads:
        copy.wait()
    for copy in small:
        copy.wait()
    width = small_weight_in.shape[-1]
    for i in range(2):
        value = small_grad_in[0, i]
        for j in range(1, n):
            value = value + small_grad_in[j, i]
        value = value * rate
        for j in range(n):
            small_full[i, j] = small_weight_in[j, i] - learn_rate * value[:, j * width : (j + 1) * width]
        small_own[i] = small_full[i, me]
    for a in range(1, 4):
        add_first(a)
    add_second(0)
    add_second(1)
    update(0)
    add_second(2)
    update(1)
    add_second(3)
    update(2)
    pass_on(0)
    update(3)
    for a in range(1, 4):
        pass_on(a)
    for copies_sent in (first, second, back, spread):
        for copy in copies_sent.values():
            copy.wait_send()
    for a in range(4):
        for copy in exchange[a][1:]:
            copy.wait_send()
    for copy in spread.values():
        copy.wait_recv()


def solution(mesh):
    n, m = mesh.shape["batch"], mesh.shape["cols"]
    n_x = math.isqrt(n)
    if n_x * n_x != n:
        n_x = n
    n_y = n // n_x
    most = max(n_x, n_y)

    def per_device(*args):
        grads, small_grads, weights, small_weights = args[0:4], args[4:6], args[6:10], args[10:12]
        width = small_weights[0].shape[0]
        blocks = [w.shape for w in weights]
        slices = blocks[0][0]
        slabs = [(b[0] // 2, b[1]) for b in blocks]
        f32, bf16 = jnp.float32, jnp.bfloat16
        DMA = pltpu.SemaphoreType.DMA
        hops = max(most - 1, 1)
        anywhere = pl.BlockSpec(memory_space=pl.ANY)
        vmem = pl.BlockSpec(memory_space=pltpu.VMEM)
        out_shape = (
            [jax.ShapeDtypeStruct(g.shape[1:], bf16) for g in grads]
            + [jax.ShapeDtypeStruct(b, f32) for b in blocks]
            + [jax.ShapeDtypeStruct((2, n, 1, width), f32), jax.ShapeDtypeStruct((2, 1, width), f32)]
        )
        results = pl.pallas_call(
            functools.partial(kernel, n, m, n_x, n_y),
            out_shape=out_shape,
            in_specs=[anywhere] * 12,
            out_specs=[vmem] * 10,
            scratch_shapes=(
                [pltpu.VMEM((2, hops, most) + s, f32) for s in slabs]
                + [pltpu.VMEM((2, hops) + s, f32) for s in slabs]
                + [pltpu.VMEM((2, most) + s, f32) for s in slabs]
                + [pltpu.VMEM(b, f32) for b in blocks]
                + [pltpu.VMEM(b, f32) for b in blocks]
                + [
                    pltpu.VMEM((4, 2, slices), f32),
                    pltpu.VMEM((4, m, 2, slices), f32),
                    pltpu.VMEM((n, 2, 1, n * width), f32),
                    pltpu.VMEM((n, 2, 1, width), f32),
                    DMA((4, 2, most)),
                    DMA((4,)),
                    DMA((4, 2, hops, most)),
                    DMA((4, 2, hops, most)),
                    DMA((4, 2, hops)),
                    DMA((4, 2, hops)),
                    DMA((4, m)),
                    DMA((4, m)),
                    DMA((4,)),
                    DMA((4, 2, hops)),
                    DMA((4, 2, hops)),
                    DMA((4, 2, hops, most)),
                    DMA((4, 2, hops, most)),
                    DMA((n, 2, 2)),
                    DMA((n, 2, 2)),
                    DMA((4,)),
                ]
            ),
            compiler_params=pltpu.CompilerParams(
                collective_id=0, has_side_effects=True, vmem_limit_bytes=40 * 2**20
            ),
        )(*grads, *small_grads, *weights, *[w.reshape(1, -1) for w in small_weights])
        full, own = results[8], results[9]
        small_copies = [full[i].reshape(-1).astype(bf16) for i in range(2)]
        small_news = [own[i].reshape(-1) for i in range(2)]
        return tuple(results[0:4]) + tuple(small_copies) + tuple(results[4:8]) + tuple(small_news)

    in_specs = (
        (P("batch", None, "cols"),) * 3
        + (P("batch", "cols", None),)
        + (P("batch", None),) * 2
        + (P("batch", "cols"),) * 3
        + (P("cols", "batch"),)
        + (P("batch"),) * 2
    )
    out_specs = (
        (P(None, "cols"),) * 3
        + (P("cols", None),)
        + (P(),) * 2
        + (P("batch", "cols"),) * 3
        + (P("cols", "batch"),)
        + (P("batch"),) * 2
    )
    return jax.shard_map(per_device, mesh=mesh, in_specs=in_specs, out_specs=out_specs, check_vma=False)
```

```python
import functools
import math

import jax
import jax.numpy as jnp
from jax import lax
from jax.experimental import pallas as pl
from jax.experimental.pallas import tpu as pltpu
from jax.sharding import PartitionSpec as P

learn_rate = 0.4
LANES = 128


def kernel(n, m, n_x, n_y, *refs):
    grads, small_grads = refs[0:4], refs[4:6]
    weights, small_weights = refs[6:10], refs[10:12]
    copies, news = refs[12:16], refs[16:20]
    small_full, small_own = refs[20:22]
    scratch = refs[22:]
    first_in, second_in, held = scratch[0:4], scratch[4:8], scratch[8:12]
    total, own_weight = scratch[12:16], scratch[16:20]
    squares, squares_in, small_grad_in, small_weight_in = scratch[20:24]
    (
        load_sem, weight_sem,
        first_send, first_recv, second_send, second_recv,
        square_send, square_recv, square_own,
        back_send, back_recv, spread_send, spread_recv,
        small_send, small_recv, small_local,
    ) = scratch[24:]
    rate = n ** (-0.5)

    me = lax.axis_index("batch")
    col = lax.axis_index("cols")
    y, x = me // n_x, lax.rem(me, n_x)

    def spot(half, d_first, d_second):
        if half == 0:
            return lax.rem(y + d_second, n_y) * n_x + lax.rem(x + d_first, n_x)
        return lax.rem(y + d_first, n_y) * n_x + lax.rem(x + d_second, n_x)

    def extents(half):
        return (n_x, n_y) if half == 0 else (n_y, n_x)

    def piece(a, ref, chunk, half):
        rows, columns = total[a].shape
        depth = rows // 2
        if a < 3:
            start = pl.multiple_of(chunk * rows + half * depth, depth)
            return ref.at[pl.ds(start, depth), :]
        start = pl.multiple_of(chunk * columns, columns)
        return ref.at[pl.ds(half * depth, depth), pl.ds(start, columns)]

    loads, weight_loads = {}, []
    for a in range(4):
        for half in range(2):
            for d in range(extents(half)[1]):
                loads[a, half, d] = pltpu.make_async_copy(
                    piece(a, grads[a].at[0], spot(half, 0, d), half),
                    held[a].at[half, d],
                    load_sem.at[a, half, d],
                )
        weight_loads.append(pltpu.make_async_copy(weights[a], own_weight[a], weight_sem.at[a]))
    small_loads = []
    for i in range(2):
        small_loads.append(pltpu.make_async_copy(small_grads[i], small_grad_in.at[me, i], small_local.at[i]))
        small_loads.append(pltpu.make_async_copy(small_weights[i], small_weight_in.at[me, i], small_local.at[2 + i]))

    barrier = pltpu.get_barrier_semaphore()
    for d in range(1, n):
        pl.semaphore_signal(barrier, inc=1, device_id={"batch": lax.rem(me + d, n)})
    for d in range(1, m):
        pl.semaphore_signal(barrier, inc=1, device_id={"cols": lax.rem(col + d, m)})
    for copy in weight_loads:
        copy.start()
    for copy in loads.values():
        copy.start()
    for copy in small_loads:
        copy.start()
    pl.semaphore_wait(barrier, n - 1 + m - 1)

    first = {}
    for a in range(4):
        for d_second in range(max(n_x, n_y) - 1, -1, -1):
            for half in range(2):
                n_first, n_second = extents(half)
                if d_second >= n_second:
                    continue
                for d_first in range(1, n_first):
                    copy = pltpu.make_async_remote_copy(
                        src_ref=piece(a, grads[a].at[0], spot(half, d_first, d_second), half),
                        dst_ref=first_in[a].at[half, d_first - 1, d_second],
                        send_sem=first_send.at[a, half, d_first - 1, d_second],
                        recv_sem=first_recv.at[a, half, d_first - 1, d_second],
                        device_id={"batch": spot(half, d_first, 0)},
                    )
                    copy.start()
                    first[a, half, d_first, d_second] = copy
        if a == 0:
            small = []
            for d in range(1, n):
                for i in range(2):
                    for k, (source, target) in enumerate(
                        ((small_grads[i], small_grad_in), (small_weights[i], small_weight_in))
                    ):
                        copy = pltpu.make_async_remote_copy(
                            src_ref=source,
                            dst_ref=target.at[me, i],
                            send_sem=small_send.at[d - 1, i, k],
                            recv_sem=small_recv.at[d - 1, i, k],
                            device_id={"batch": lax.rem(me + d, n)},
                        )
                        copy.start()
                        small.append(copy)

    def row_squares(a, value):
        value = value * value
        if a == 3:
            return jnp.sum(value, axis=0, keepdims=True)
        folded = value[:, :LANES]
        for start in range(LANES, value.shape[1], LANES):
            folded = folded + value[:, start : start + LANES]
        return jnp.sum(folded.T, axis=0, keepdims=True)

    for a in range(4):
        weight_loads[a].wait()
        squares[a, 0:1] = row_squares(a, own_weight[a][...])

    second = {}

    def add_first(a):
        for d_second in range(max(n_x, n_y) - 1, -1, -1):
            for half in range(2):
                n_first, n_second = extents(half)
                if d_second >= n_second:
                    continue
                loads[a, half, d_second].wait()
                value = held[a][half, d_second]
                for d_first in range(1, n_first):
                    first[a, half, d_first, d_second].wait_recv()
                    value = value + first_in[a][half, d_first - 1, d_second]
                held[a][half, d_second] = value
                if d_second > 0:
                    copy = pltpu.make_async_remote_copy(
                        src_ref=held[a].at[half, d_second],
                        dst_ref=second_in[a].at[half, d_second - 1],
                        send_sem=second_send.at[a, half, d_second - 1],
                        recv_sem=second_recv.at[a, half, d_second - 1],
                        device_id={"batch": spot(half, 0, d_second)},
                    )
                    copy.start()
                    second[a, half, d_second] = copy

    exchange = {}

    def add_second(a):
        depth = total[a].shape[0] // 2
        for half in range(2):
            value = held[a][half, 0]
            for d_second in range(1, extents(half)[1]):
                second[a, half, d_second].wait_recv()
                value = value + second_in[a][half, d_second - 1]
            total[a][half * depth : (half + 1) * depth] = value * rate
        squares[a, 1:2] = row_squares(a, total[a][...])
        own = pltpu.make_async_copy(squares.at[a], squares_in.at[a, col], square_own.at[a])
        exchange[a] = [own]
        for d in range(1, m):
            copy = pltpu.make_async_remote_copy(
                src_ref=squares.at[a],
                dst_ref=squares_in.at[a, col],
                send_sem=square_send.at[a, d - 1],
                recv_sem=square_recv.at[a, d - 1],
                device_id={"cols": lax.rem(col + d, m)},
            )
            copy.start()
            exchange[a].append(copy)
        own.start()

    back, spread = {}, {}

    def send_spread(a, half, d_second):
        n_first, n_second = extents(half)
        slab = piece(a, copies[a], spot(half, 0, n_second - d_second), half)
        for d_first in range(1, n_first):
            copy = pltpu.make_async_remote_copy(
                src_ref=slab,
                dst_ref=slab,
                send_sem=spread_send.at[a, half, d_first - 1, d_second],
                recv_sem=spread_recv.at[a, half, d_first - 1, d_second],
                device_id={"batch": spot(half, d_first, 0)},
            )
            copy.start()
            spread[a, half, d_first, d_second] = copy

    def update(a):
        exchange[a][0].wait()
        for copy in exchange[a][1:]:
            copy.wait_recv()
        both = squares_in[a, 0]
        for d in range(1, m):
            both = both + squares_in[a, d]
        ratio = learn_rate * (jnp.sqrt(both[0:1]) * lax.rsqrt(both[1:2] + 1e-06))
        rows, columns = total[a].shape
        if a < 3:
            ratio = jnp.broadcast_to(ratio, (LANES, rows)).T
            for start in range(0, columns, LANES):
                block = slice(start, start + LANES)
                news[a][:, block] = own_weight[a][:, block] - total[a][:, block] * ratio
        else:
            news[a][...] = own_weight[a][...] - total[a][...] * ratio
        depth = rows // 2
        for half in range(2):
            piece(a, copies[a], me, half)[...] = news[a][half * depth : (half + 1) * depth].astype(jnp.bfloat16)
        for half in range(2):
            slab = piece(a, copies[a], me, half)
            for d_second in range(1, extents(half)[1]):
                copy = pltpu.make_async_remote_copy(
                    src_ref=slab,
                    dst_ref=slab,
                    send_sem=back_send.at[a, half, d_second - 1],
                    recv_sem=back_recv.at[a, half, d_second - 1],
                    device_id={"batch": spot(half, 0, d_second)},
                )
                copy.start()
                back[a, half, d_second] = copy
            send_spread(a, half, 0)

    def pass_on(a):
        for half in range(2):
            for d_second in range(1, extents(half)[1]):
                back[a, half, d_second].wait_recv()
                send_spread(a, half, d_second)

    add_first(0)
    for copy in small_loads:
        copy.wait()
    for copy in small:
        copy.wait()
    width = small_weight_in.shape[-1]
    for i in range(2):
        value = small_grad_in[0, i]
        for j in range(1, n):
            value = value + small_grad_in[j, i]
        value = value * rate
        for j in range(n):
            small_full[i, j] = small_weight_in[j, i] - learn_rate * value[:, j * width : (j + 1) * width]
        small_own[i] = small_full[i, me]
    for a in range(1, 4):
        add_first(a)
    add_second(0)
    add_second(1)
    update(0)
    add_second(2)
    update(1)
    add_second(3)
    update(2)
    pass_on(0)
    update(3)
    for a in range(1, 4):
        pass_on(a)
    for copies_sent in (first, second, back, spread):
        for copy in copies_sent.values():
            copy.wait_send()
    for a in range(4):
        for copy in exchange[a][1:]:
            copy.wait_send()
    for copy in spread.values():
        copy.wait_recv()


def finish(n, *refs):
    results, full, own = refs[0:8], refs[8], refs[9]
    outs, small_copies, small_news = refs[10:18], refs[18:20], refs[20:22]
    copy_rows, new_rows, sem, small_sem = refs[22:24], refs[24:26], refs[26], refs[27]
    moves = [pltpu.make_async_copy(results[i], outs[i], sem.at[i]) for i in range(8)]
    for move in moves:
        move.start()
    width = full.shape[-1]
    for i in range(2):
        for j in range(n):
            copy_rows[i][j * width : (j + 1) * width] = full[i, j, 0].astype(jnp.bfloat16)
        new_rows[i][...] = own[i, 0]
    for i in range(2):
        moves.append(pltpu.make_async_copy(copy_rows[i], small_copies[i], small_sem.at[i]))
        moves.append(pltpu.make_async_copy(new_rows[i], small_news[i], small_sem.at[2 + i]))
    for move in moves[8:]:
        move.start()
    for move in moves:
        move.wait()


def solution(mesh):
    n, m = mesh.shape["batch"], mesh.shape["cols"]
    n_x = math.isqrt(n)
    if n_x * n_x != n:
        n_x = n
    n_y = n // n_x
    most = max(n_x, n_y)

    def per_device(*args):
        args = args[:10] + tuple(w.reshape(1, -1) for w in args[10:])
        grads, weights, width = args[0:4], args[6:10], args[10].shape[1]
        blocks = [w.shape for w in weights]
        slices = blocks[0][0]
        slabs = [(b[0] // 2, b[1]) for b in blocks]
        f32, bf16 = jnp.float32, jnp.bfloat16
        DMA = pltpu.SemaphoreType.DMA
        hops = max(most - 1, 1)
        hbm = pl.BlockSpec(memory_space=pltpu.HBM)
        vmem = pl.BlockSpec(memory_space=pltpu.VMEM)
        out_shape = (
            [jax.ShapeDtypeStruct(g.shape[1:], bf16) for g in grads]
            + [jax.ShapeDtypeStruct(b, f32) for b in blocks]
            + [jax.ShapeDtypeStruct((2, n, 1, width), f32), jax.ShapeDtypeStruct((2, 1, width), f32)]
        )
        results = pl.pallas_call(
            functools.partial(kernel, n, m, n_x, n_y),
            out_shape=[pltpu.VMEM(o.shape, o.dtype) for o in out_shape],
            in_specs=[hbm] * 12,
            out_specs=[vmem] * 10,
            scratch_shapes=(
                [pltpu.VMEM((2, hops, most) + s, f32) for s in slabs]
                + [pltpu.VMEM((2, hops) + s, f32) for s in slabs]
                + [pltpu.VMEM((2, most) + s, f32) for s in slabs]
                + [pltpu.VMEM(b, f32) for b in blocks]
                + [pltpu.VMEM(b, f32) for b in blocks]
                + [
                    pltpu.VMEM((4, 2, slices), f32),
                    pltpu.VMEM((4, m, 2, slices), f32),
                    pltpu.VMEM((n, 2, 1, n * width), f32),
                    pltpu.VMEM((n, 2, 1, width), f32),
                    DMA((4, 2, most)),
                    DMA((4,)),
                    DMA((4, 2, hops, most)),
                    DMA((4, 2, hops, most)),
                    DMA((4, 2, hops)),
                    DMA((4, 2, hops)),
                    DMA((4, m)),
                    DMA((4, m)),
                    DMA((4,)),
                    DMA((4, 2, hops)),
                    DMA((4, 2, hops)),
                    DMA((4, 2, hops, most)),
                    DMA((4, 2, hops, most)),
                    DMA((n, 2, 2)),
                    DMA((n, 2, 2)),
                    DMA((4,)),
                ]
            ),
            compiler_params=pltpu.CompilerParams(
                collective_id=0, has_side_effects=True, vmem_limit_bytes=40 * 2**20
            ),
        )(*[pltpu.with_memory_space_constraint(v, pltpu.HBM) for v in args])
        done = pl.pallas_call(
            functools.partial(finish, n),
            out_shape=out_shape[:8]
            + [jax.ShapeDtypeStruct((n * width,), bf16)] * 2
            + [jax.ShapeDtypeStruct((width,), f32)] * 2,
            in_specs=[vmem] * 10,
            out_specs=[hbm] * 12,
            scratch_shapes=[pltpu.VMEM((n * width,), bf16)] * 2
            + [pltpu.VMEM((width,), f32)] * 2
            + [DMA((8,)), DMA((4,))],
            compiler_params=pltpu.CompilerParams(vmem_limit_bytes=2**20),
        )(*results)
        return tuple(done[0:4]) + tuple(done[8:10]) + tuple(done[4:8]) + tuple(done[10:12])

    in_specs = (
        (P("batch", None, "cols"),) * 3
        + (P("batch", "cols", None),)
        + (P("batch", None),) * 2
        + (P("batch", "cols"),) * 3
        + (P("cols", "batch"),)
        + (P("batch"),) * 2
    )
    out_specs = (
        (P(None, "cols"),) * 3
        + (P("cols", None),)
        + (P(),) * 2
        + (P("batch", "cols"),) * 3
        + (P("cols", "batch"),)
        + (P("batch"),) * 2
    )
    return jax.shard_map(per_device, mesh=mesh, in_specs=in_specs, out_specs=out_specs, check_vma=False)
```

```python
import functools
import math

import jax
import jax.numpy as jnp
from jax import lax
from jax.experimental import pallas as pl
from jax.experimental.pallas import tpu as pltpu
from jax.sharding import PartitionSpec as P

learn_rate = 0.4
LANES = 128
ORDER = (
    ("F0", "F1", "S", "W0", "W1", "W2", "W3", "A0", "F2", "A1", "F3", "N", "B0")
    + ("A2", "B1", "U0", "A3", "B2", "U1", "P0", "B3", "U2", "P1", "U3", "P2", "P3")
)


def kernel(n, m, n_x, n_y, *refs):
    grads, small_grads = refs[0:4], refs[4:6]
    weights, small_weights = refs[6:10], refs[10:12]
    copies, news = refs[12:16], refs[16:20]
    small_full, small_own = refs[20:22]
    scratch = refs[22:]
    first_in, second_in, held = scratch[0:4], scratch[4:8], scratch[8:12]
    total, own_weight = scratch[12:16], scratch[16:20]
    squares, squares_in, small_in = scratch[20:23]
    (
        load_sem, weight_sem,
        first_send, first_recv, second_send, second_recv,
        square_send, square_recv, square_own,
        back_send, back_recv, spread_send, spread_recv,
        small_send, small_recv, small_local,
    ) = scratch[23:]
    rate = n ** (-0.5)

    me = lax.axis_index("batch")
    col = lax.axis_index("cols")
    y, x = me // n_x, lax.rem(me, n_x)

    def spot(half, d_first, d_second):
        if half == 0:
            return lax.rem(y + d_second, n_y) * n_x + lax.rem(x + d_first, n_x)
        return lax.rem(y + d_first, n_y) * n_x + lax.rem(x + d_second, n_x)

    def extents(half):
        return (n_x, n_y) if half == 0 else (n_y, n_x)

    def piece(a, ref, chunk, half):
        rows, columns = total[a].shape
        depth = rows // 2
        if a < 3:
            start = pl.multiple_of(chunk * rows + half * depth, depth)
            return ref.at[pl.ds(start, depth), :]
        start = pl.multiple_of(chunk * columns, columns)
        return ref.at[pl.ds(half * depth, depth), pl.ds(start, columns)]

    loads, weight_loads = {}, []
    for a in range(4):
        for half in range(2):
            for d in range(extents(half)[1]):
                loads[a, half, d] = pltpu.make_async_copy(
                    piece(a, grads[a].at[0], spot(half, 0, d), half),
                    held[a].at[half, d],
                    load_sem.at[a, half, d],
                )
        weight_loads.append(pltpu.make_async_copy(weights[a], own_weight[a], weight_sem.at[a]))
    small_loads, width = [], small_weights[0].shape[1]
    for i in range(2):
        small_loads.append(
            pltpu.make_async_copy(small_grads[i], small_in.at[me, :, pl.ds(i * n * width, n * width)], small_local.at[i])
        )
        small_loads.append(
            pltpu.make_async_copy(
                small_weights[i], small_in.at[me, :, pl.ds((2 * n + i) * width, width)], small_local.at[2 + i]
            )
        )

    barrier = pltpu.get_barrier_semaphore()
    for d in range(1, n):
        pl.semaphore_signal(barrier, inc=1, device_id={"batch": lax.rem(me + d, n)})
    for d in range(1, m):
        pl.semaphore_signal(barrier, inc=1, device_id={"cols": lax.rem(col + d, m)})
    for copy in small_loads:
        copy.start()
    for copy in weight_loads:
        copy.start()
    for copy in loads.values():
        copy.start()
    pl.semaphore_wait(barrier, n - 1 + m - 1)

    first, small = {}, []

    def send_first(a):
        for d_second in range(max(n_x, n_y) - 1, -1, -1):
            for half in range(2):
                n_first, n_second = extents(half)
                if d_second >= n_second:
                    continue
                for d_first in range(1, n_first):
                    copy = pltpu.make_async_remote_copy(
                        src_ref=piece(a, grads[a].at[0], spot(half, d_first, d_second), half),
                        dst_ref=first_in[a].at[half, d_first - 1, d_second],
                        send_sem=first_send.at[a, half, d_first - 1, d_second],
                        recv_sem=first_recv.at[a, half, d_first - 1, d_second],
                        device_id={"batch": spot(half, d_first, 0)},
                    )
                    copy.start()
                    first[a, half, d_first, d_second] = copy

    def send_small():
        for copy in small_loads:
            copy.wait()
        for d in range(1, n):
            copy = pltpu.make_async_remote_copy(
                src_ref=small_in.at[me],
                dst_ref=small_in.at[me],
                send_sem=small_send.at[d - 1],
                recv_sem=small_recv.at[d - 1],
                device_id={"batch": lax.rem(me + d, n)},
            )
            copy.start()
            small.append(copy)

    def row_squares(a, value):
        value = value * value
        if a == 3:
            return jnp.sum(value, axis=0, keepdims=True)
        folded = value[:, :LANES]
        for start in range(LANES, value.shape[1], LANES):
            folded = folded + value[:, start : start + LANES]
        return jnp.sum(folded.T, axis=0, keepdims=True)

    def weigh(a):
        weight_loads[a].wait()
        squares[a, 0:1] = row_squares(a, own_weight[a][...])

    second = {}

    def add_first(a):
        for d_second in range(max(n_x, n_y) - 1, -1, -1):
            for half in range(2):
                n_first, n_second = extents(half)
                if d_second >= n_second:
                    continue
                loads[a, half, d_second].wait()
                value = held[a][half, d_second]
                for d_first in range(1, n_first):
                    first[a, half, d_first, d_second].wait_recv()
                    value = value + first_in[a][half, d_first - 1, d_second]
                held[a][half, d_second] = value
                if d_second > 0:
                    copy = pltpu.make_async_remote_copy(
                        src_ref=held[a].at[half, d_second],
                        dst_ref=second_in[a].at[half, d_second - 1],
                        send_sem=second_send.at[a, half, d_second - 1],
                        recv_sem=second_recv.at[a, half, d_second - 1],
                        device_id={"batch": spot(half, 0, d_second)},
                    )
                    copy.start()
                    second[a, half, d_second] = copy

    exchange = {}

    def add_second(a):
        depth = total[a].shape[0] // 2
        for half in range(2):
            value = held[a][half, 0]
            for d_second in range(1, extents(half)[1]):
                second[a, half, d_second].wait_recv()
                value = value + second_in[a][half, d_second - 1]
            total[a][half * depth : (half + 1) * depth] = value * rate
        squares[a, 1:2] = row_squares(a, total[a][...])
        own = pltpu.make_async_copy(squares.at[a], squares_in.at[a, col], square_own.at[a])
        exchange[a] = [own]
        for d in range(1, m):
            copy = pltpu.make_async_remote_copy(
                src_ref=squares.at[a],
                dst_ref=squares_in.at[a, col],
                send_sem=square_send.at[a, d - 1],
                recv_sem=square_recv.at[a, d - 1],
                device_id={"cols": lax.rem(col + d, m)},
            )
            copy.start()
            exchange[a].append(copy)
        own.start()

    back, spread = {}, {}

    def send_spread(a, half, d_second):
        n_first, n_second = extents(half)
        slab = piece(a, copies[a], spot(half, 0, n_second - d_second), half)
        for d_first in range(1, n_first):
            copy = pltpu.make_async_remote_copy(
                src_ref=slab,
                dst_ref=slab,
                send_sem=spread_send.at[a, half, d_first - 1, d_second],
                recv_sem=spread_recv.at[a, half, d_first - 1, d_second],
                device_id={"batch": spot(half, d_first, 0)},
            )
            copy.start()
            spread[a, half, d_first, d_second] = copy

    def update(a):
        exchange[a][0].wait()
        for copy in exchange[a][1:]:
            copy.wait_recv()
        both = squares_in[a, 0]
        for d in range(1, m):
            both = both + squares_in[a, d]
        ratio = learn_rate * (jnp.sqrt(both[0:1]) * lax.rsqrt(both[1:2] + 1e-06))
        rows, columns = total[a].shape
        if a < 3:
            ratio = jnp.broadcast_to(ratio, (LANES, rows)).T
            for start in range(0, columns, LANES):
                block = slice(start, start + LANES)
                news[a][:, block] = own_weight[a][:, block] - total[a][:, block] * ratio
        else:
            news[a][...] = own_weight[a][...] - total[a][...] * ratio
        depth = rows // 2
        for half in range(2):
            piece(a, copies[a], me, half)[...] = news[a][half * depth : (half + 1) * depth].astype(jnp.bfloat16)
        for half in range(2):
            slab = piece(a, copies[a], me, half)
            for d_second in range(1, extents(half)[1]):
                copy = pltpu.make_async_remote_copy(
                    src_ref=slab,
                    dst_ref=slab,
                    send_sem=back_send.at[a, half, d_second - 1],
                    recv_sem=back_recv.at[a, half, d_second - 1],
                    device_id={"batch": spot(half, 0, d_second)},
                )
                copy.start()
                back[a, half, d_second] = copy
            send_spread(a, half, 0)

    def pass_on(a):
        for half in range(2):
            for d_second in range(1, extents(half)[1]):
                back[a, half, d_second].wait_recv()
                send_spread(a, half, d_second)

    def update_small():
        for copy in small:
            copy.wait()
        for i in range(2):
            value = small_in[0, :, i * n * width : (i + 1) * n * width]
            for j in range(1, n):
                value = value + small_in[j, :, i * n * width : (i + 1) * n * width]
            value = value * rate
            for j in range(n):
                weight = small_in[j, :, (2 * n + i) * width : (2 * n + i + 1) * width]
                small_full[i, j] = weight - learn_rate * value[:, j * width : (j + 1) * width]
            small_own[i] = small_full[i, me]

    steps = dict(
        F=send_first, S=send_small, W=weigh, A=add_first, N=update_small, B=add_second, U=update, P=pass_on
    )
    for step in ORDER:
        steps[step[0]](*map(int, step[1:]))
    for copies_sent in (first, second, back, spread):
        for copy in copies_sent.values():
            copy.wait_send()
    for a in range(4):
        for copy in exchange[a][1:]:
            copy.wait_send()
    for copy in spread.values():
        copy.wait_recv()


def finish(n, *refs):
    results, full, own = refs[0:8], refs[8], refs[9]
    outs, small_copies, small_news = refs[10:18], refs[18:20], refs[20:22]
    copy_rows, new_rows, sem, small_sem = refs[22:24], refs[24:26], refs[26], refs[27]
    moves = [pltpu.make_async_copy(results[i], outs[i], sem.at[i]) for i in range(8)]
    for move in moves:
        move.start()
    width = full.shape[-1]
    for i in range(2):
        for j in range(n):
            copy_rows[i][j * width : (j + 1) * width] = full[i, j, 0].astype(jnp.bfloat16)
        new_rows[i][...] = own[i, 0]
    for i in range(2):
        moves.append(pltpu.make_async_copy(copy_rows[i], small_copies[i], small_sem.at[i]))
        moves.append(pltpu.make_async_copy(new_rows[i], small_news[i], small_sem.at[2 + i]))
    for move in moves[8:]:
        move.start()
    for move in moves:
        move.wait()


def solution(mesh):
    n, m = mesh.shape["batch"], mesh.shape["cols"]
    n_x = math.isqrt(n)
    if n_x * n_x != n:
        n_x = n
    n_y = n // n_x
    most = max(n_x, n_y)

    def per_device(*args):
        args = args[:10] + tuple(w.reshape(1, -1) for w in args[10:])
        grads, weights, width = args[0:4], args[6:10], args[10].shape[1]
        blocks = [w.shape for w in weights]
        slices = blocks[0][0]
        slabs = [(b[0] // 2, b[1]) for b in blocks]
        f32, bf16 = jnp.float32, jnp.bfloat16
        DMA = pltpu.SemaphoreType.DMA
        hops = max(most - 1, 1)
        hbm = pl.BlockSpec(memory_space=pltpu.HBM)
        vmem = pl.BlockSpec(memory_space=pltpu.VMEM)
        out_shape = (
            [jax.ShapeDtypeStruct(g.shape[1:], bf16) for g in grads]
            + [jax.ShapeDtypeStruct(b, f32) for b in blocks]
            + [jax.ShapeDtypeStruct((2, n, 1, width), f32), jax.ShapeDtypeStruct((2, 1, width), f32)]
        )
        results = pl.pallas_call(
            functools.partial(kernel, n, m, n_x, n_y),
            out_shape=[pltpu.VMEM(o.shape, o.dtype) for o in out_shape],
            in_specs=[hbm] * 12,
            out_specs=[vmem] * 10,
            scratch_shapes=(
                [pltpu.VMEM((2, hops, most) + s, f32) for s in slabs]
                + [pltpu.VMEM((2, hops) + s, f32) for s in slabs]
                + [pltpu.VMEM((2, most) + s, f32) for s in slabs]
                + [pltpu.VMEM(b, f32) for b in blocks]
                + [pltpu.VMEM(b, f32) for b in blocks]
                + [
                    pltpu.VMEM((4, 2, slices), f32),
                    pltpu.VMEM((4, m, 2, slices), f32),
                    pltpu.VMEM((n, 1, 2 * (n + 1) * width), f32),
                    DMA((4, 2, most)),
                    DMA((4,)),
                    DMA((4, 2, hops, most)),
                    DMA((4, 2, hops, most)),
                    DMA((4, 2, hops)),
                    DMA((4, 2, hops)),
                    DMA((4, m)),
                    DMA((4, m)),
                    DMA((4,)),
                    DMA((4, 2, hops)),
                    DMA((4, 2, hops)),
                    DMA((4, 2, hops, most)),
                    DMA((4, 2, hops, most)),
                    DMA((n,)),
                    DMA((n,)),
                    DMA((4,)),
                ]
            ),
            compiler_params=pltpu.CompilerParams(
                collective_id=0, has_side_effects=True, vmem_limit_bytes=40 * 2**20
            ),
        )(*[pltpu.with_memory_space_constraint(v, pltpu.HBM) for v in args])
        done = pl.pallas_call(
            functools.partial(finish, n),
            out_shape=out_shape[:8]
            + [jax.ShapeDtypeStruct((n * width,), bf16)] * 2
            + [jax.ShapeDtypeStruct((width,), f32)] * 2,
            in_specs=[vmem] * 10,
            out_specs=[hbm] * 12,
            scratch_shapes=[pltpu.VMEM((n * width,), bf16)] * 2
            + [pltpu.VMEM((width,), f32)] * 2
            + [DMA((8,)), DMA((4,))],
            compiler_params=pltpu.CompilerParams(vmem_limit_bytes=2**20),
        )(*results)
        return tuple(done[0:4]) + tuple(done[8:10]) + tuple(done[4:8]) + tuple(done[10:12])

    in_specs = (
        (P("batch", None, "cols"),) * 3
        + (P("batch", "cols", None),)
        + (P("batch", None),) * 2
        + (P("batch", "cols"),) * 3
        + (P("cols", "batch"),)
        + (P("batch"),) * 2
    )
    out_specs = (
        (P(None, "cols"),) * 3
        + (P("cols", None),)
        + (P(),) * 2
        + (P("batch", "cols"),) * 3
        + (P("cols", "batch"),)
        + (P("batch"),) * 2
    )
    return jax.shard_map(per_device, mesh=mesh, in_specs=in_specs, out_specs=out_specs, check_vma=False)
```
